32 devices in a mesh: node: 4 (over y, core), rep: 8 (over z, x).
Axes of the slice: x: 2, y: 2, z: 4, core: 2. Of those that a mesh axis runs over, the one named last changes fastest.
Arguments:
- tokens: bfloat16 [8192, 2048], P(('node', 'rep')), may hold values from -60 to 60
- cotangent: bfloat16 [8192, 512], P(('node', 'rep')), may hold values from -6 to 6
- value_weight: bfloat16 [2048, 512], P('node'), may hold values from -0.25 to 0.25
Outputs:
- input_grad: bfloat16 [8192, 2048], P(('node', 'rep'))
- update: float32 [2048, 512], P('node')
The draws below stay inside these ranges and needn't reach their ends.
All inputs are finite; a program needn't handle non-finite values.
Results may differ from the reference program's by a relative error of at most 0.025.
Values may be sent and summed in bfloat16 or wider, within the bound.
No kernel may reach another device: no remote copies, remote signals or barrier semaphores. Data moves between devices by JAX's collectives and lax.ppermute only.
A program may use at most 64 MiB of HBM per device.

```python
import math
import jax
import jax.numpy as jnp
from jax import lax

DIN = 2048
KVH = 4
HD = 128
NS_ITERS = 5
TOK_DEV = 256
CV = 512
TOKENS = 8192
N_NODE = 4


def draw_tokens(key, part):
    key_values = jax.random.fold_in(key, 11)
    key_rough = jax.random.fold_in(key, 12)
    key_pair = jax.random.fold_in(key, 13)
    columns = jnp.arange(DIN, dtype=jnp.float32) / (DIN - 1)
    rough = jnp.exp(jax.random.uniform(key_rough, (DIN,), jnp.float32, jnp.log(0.7), jnp.log(1.4)))
    values = jnp.clip(jax.random.normal(key_values, (TOKENS, DIN), jnp.float32), -6.0, 6.0)
    rise = 3.0 ** columns
    offset = jax.random.randint(key_pair, (), 0, N_NODE)
    row_block = jnp.arange(TOKENS, dtype=jnp.int32) // TOK_DEV
    col_block = jnp.arange(DIN, dtype=jnp.int32) // (DIN // N_NODE)
    paired = ((row_block + offset) % N_NODE)[:, None] == col_block[None, :]
    spike = jnp.where(paired, 3.0, 1.0).astype(jnp.float32)
    return (values * spike * (rise * rough)[None, :]).astype(jnp.bfloat16)


def shard_levels(own_key, dims, pieces, smallest, high):
    loudness, own = 1.0, jax.random.fold_in(own_key, 6)
    for position, shards_of in pieces:
        draws = jnp.exp(jax.random.uniform(jax.random.fold_in(own, position), (shards_of,), jnp.float32, smallest / len(pieces), high / len(pieces)))
        loudness = loudness * jnp.repeat(draws, dims[position] // shards_of).reshape([-1 if axis == position else 1 for axis in range(len(dims))])
    return loudness


def noise(key, extent, deviation, most, split=(), kind=jnp.bfloat16):
    drawn = jax.random.normal(key, extent, jnp.float32) * deviation
    if len(split) > 0:
        drawn = shard_levels(key, extent, split, -0.22, 0.18) * drawn
    return jnp.clip(drawn, min=-most, max=most).astype(kind)


def setup_inputs(seed: int = 0) -> dict:
    seeds = jax.random.split(jax.random.key(seed), 4)
    tokens = draw_tokens(jax.random.fold_in(seeds[3], 71), 0)
    cotangent = noise(seeds[1], (TOKENS, CV), 1.0, 6.0, ((0, 32),))
    value_weight = noise(seeds[2], (DIN, CV), CV ** -0.5, 0.25, ((0, 4),))
    return {"tokens": tokens, "cotangent": cotangent, "value_weight": value_weight}


coef_a = 3.4445
coef_b = -4.775
coef_c = 2.0315
epsilon = 1e-07

def block_term(total, pair):
    rows_x, rows_c = pair
    term = jnp.einsum('td,tc->dc', rows_x.astype(jnp.float32), rows_c.astype(jnp.float32), precision=lax.Precision.HIGHEST)
    rounded = lax.optimization_barrier(term.astype(jnp.bfloat16))
    return (total + rounded.astype(jnp.float32), None)

def reference(tokens, cotangent, value_weight):
    width = cotangent.shape[1]
    input_grad = jnp.dot(cotangent, value_weight.T, preferred_element_type=jnp.float32).astype(jnp.bfloat16)
    blocks_x = tokens.reshape(-1, TOK_DEV, DIN)
    blocks_c = cotangent.reshape(-1, TOK_DEV, width)
    gradient, unused = lax.scan(block_term, jnp.zeros((DIN, width), jnp.float32), (blocks_x, blocks_c))
    blocks = gradient.reshape(DIN, KVH, HD)
    norms = jnp.sqrt(lax.optimization_barrier(jnp.sum(blocks * blocks, axis=(0, 2))))
    iterate = blocks / (norms[None, :, None] + epsilon)
    for step in range(NS_ITERS):
        gram = jnp.einsum('rhi,rhj->hij', iterate, iterate, precision=lax.Precision.HIGHEST)
        poly = coef_b * gram + coef_c * jnp.einsum('hij,hjk->hik', gram, gram, precision=lax.Precision.HIGHEST)
        iterate = coef_a * iterate + jnp.einsum('rhi,hij->rhj', iterate, poly, precision=lax.Precision.HIGHEST)
    update = 0.2 * math.sqrt(DIN) * iterate.reshape(DIN, width)
    return (input_grad, update)
```

```python
import math

import jax
import jax.numpy as jnp
from jax import lax
from jax.experimental import pallas as pl
from jax.experimental.pallas import tpu as pltpu
from jax.sharding import PartitionSpec as P

DIN = 2048
HD = 128
NS_ITERS = 5
CORES = 2
LANES = 128

coef_a = 3.4445
coef_b = -4.775
coef_c = 2.0315
epsilon = 1e-07


F32 = jnp.float32
BF16 = jnp.bfloat16
NT = (((1,), (1,)), ((), ()))
NN = (((1,), (0,)), ((), ()))


def plain(tokens, cotangent, value_weight):
    width = value_weight.shape[1]
    local_rows = value_weight.shape[0]
    heads = width // HD
    input_grad = lax.dot_general(
        cotangent,
        lax.all_gather(value_weight, "node", axis=0, tiled=True),
        (((1,), (1,)), ((), ())),
        preferred_element_type=jnp.float32,
    ).astype(jnp.bfloat16)
    partial_rows = lax.psum_scatter(
        lax.dot_general(
            tokens, cotangent, (((0,), (0,)), ((), ())), preferred_element_type=jnp.float32
        ).astype(jnp.bfloat16),
        "node",
        scatter_dimension=0,
        tiled=True,
    ).astype(jnp.float32)
    gradient = lax.psum(partial_rows, "rep")
    blocks = gradient.reshape(local_rows, heads, HD)
    local_raw = jnp.einsum("rhi,rhj->hij", blocks, blocks, precision=lax.Precision.HIGHEST)
    gram_raw = lax.psum(local_raw, "node")
    squares = jnp.einsum("hii->h", gram_raw)
    divisor = jnp.sqrt(squares) + epsilon
    start_iterate = blocks / divisor[None, :, None]
    gram = gram_raw / (divisor * divisor)[:, None, None]
    identity = jnp.broadcast_to(jnp.eye(HD, dtype=jnp.float32), (heads, HD, HD))
    total = identity
    for step in range(NS_ITERS):
        factor = (
            coef_a * identity
            + coef_b * gram
            + coef_c * jnp.einsum("hij,hjk->hik", gram, gram, precision=lax.Precision.HIGHEST)
        )
        total = jnp.einsum("hij,hjk->hik", total, factor, precision=lax.Precision.HIGHEST)
        if step + 1 < NS_ITERS:
            halfway = jnp.einsum("hij,hjk->hik", gram, factor, precision=lax.Precision.HIGHEST)
            gram = jnp.einsum("hji,hjk->hik", factor, halfway, precision=lax.Precision.HIGHEST)
    iterate = jnp.einsum("rhi,hij->rhj", start_iterate, total, precision=lax.Precision.HIGHEST)
    update = 0.2 * math.sqrt(DIN) * iterate.reshape(local_rows, width)
    return (input_grad, update)


def kernel_call(body, outs, scalars, arrays, scratch=(), flops=0):
    specs = [pl.BlockSpec(memory_space=pltpu.SMEM)]
    specs += [pl.BlockSpec(memory_space=pltpu.VMEM) for unused in arrays]
    return pl.pallas_call(
        body,
        out_shape=[jax.ShapeDtypeStruct(shape, kind) for shape, kind in outs],
        in_specs=specs,
        out_specs=[pl.BlockSpec(memory_space=pltpu.VMEM) for unused in outs],
        scratch_shapes=list(scratch),
        cost_estimate=pl.CostEstimate(flops=flops, transcendentals=0, bytes_accessed=0),
    )(scalars, *arrays)


def exact_dot(left, right, dims=NN):
    return lax.dot_general(
        left, right, dims, precision=lax.Precision.HIGHEST, preferred_element_type=F32
    )


def exchanged(mesh):
    nodes, reps = mesh.shape["node"], mesh.shape["rep"]

    def per_device(tokens, cotangent, value_weight):
        din, width = tokens.shape[1], cotangent.shape[1]
        local_rows = value_weight.shape[0]
        heads = width // HD
        n_y, n_z = nodes // CORES, heads
        n_x = reps // n_z
        piece = local_rows // n_x
        n, r = lax.axis_index("node"), lax.axis_index("rep")
        core, y = n % CORES, n // CORES
        z, x = r // n_x, r % n_x

        def send(value, my=0, mz=0, mx=0, mc=0):
            pairs = []
            for nn in range(nodes):
                for rr in range(reps):
                    ty = (nn // CORES + my) % n_y
                    tc = (nn % CORES + mc) % CORES
                    tz = (rr // n_x + mz) % n_z
                    tx = (rr % n_x + mx) % n_x
                    pairs.append((nn * reps + rr, (ty * CORES + tc) * reps + tz * n_x + tx))
            return lax.ppermute(value, ("node", "rep"), pairs)

        yx = [(my, mx) for my in range(n_y) for mx in range(n_x)]

        def dest(base, shift, size):
            return (base + shift) % size

        def source(base, shift, size):
            return (base - shift) % size

        tokens_other = send(tokens, mc=1)
        cotangent_other = send(cotangent, mc=1)
        weight_part = lax.dynamic_slice_in_dim(value_weight, x * piece, piece, 0)
        weight_far = {my: send(weight_part, my=my) for my in range(1, n_y)}

        where = jnp.stack(
            [(dest(y, my, n_y) * CORES + core) * local_rows + dest(x, mx, n_x) * piece for my, mx in yx]
        ).astype(jnp.int32)

        def term_body(at, tok_a, tok_b, cot_a, cot_b, *outs):
            left_a = cot_a[...].T
            left_b = cot_b[...].T
            for k, out in enumerate(outs):
                start = pl.multiple_of(at[k], LANES)
                block = lax.dot_general(
                    left_a, tok_a[:, pl.ds(start, piece)], NN, preferred_element_type=F32
                )
                block += lax.dot_general(
                    left_b, tok_b[:, pl.ds(start, piece)], NN, preferred_element_type=F32
                )
                out[...] = block.astype(BF16)

        terms = kernel_call(
            term_body,
            [((width, piece), BF16) for unused in yx],
            where,
            [tokens, tokens_other, cotangent, cotangent_other],
            flops=4 * tokens.shape[0] * width * piece * len(yx),
        )
        arrived = [
            terms[k] if (my, mx) == (0, 0) else send(terms[k], my=my, mx=mx) for k, (my, mx) in enumerate(yx)
        ]

        head_at = jnp.stack([dest(z, mz, n_z) * HD for mz in range(n_z)]).astype(jnp.int32)

        def sum_yx_body(at, *refs):
            ins, outs = refs[: len(yx)], refs[len(yx) :]
            for mz, out in enumerate(outs):
                rows = pl.ds(pl.multiple_of(at[mz], HD), HD)
                total = ins[0][rows, :].astype(F32)
                for ref in ins[1:]:
                    total += ref[rows, :].astype(F32)
                out[...] = total.astype(BF16)

        by_head = kernel_call(
            sum_yx_body, [((HD, piece), BF16) for unused in range(n_z)], head_at, arrived, flops=10**6
        )
        own_head = [by_head[0]] + [send(by_head[mz], mz=mz) for mz in range(1, n_z)]

        def sum_z_body(at, *refs):
            ins, (flat, tall) = refs[:n_z], refs[n_z:]
            total = ins[0][...].astype(F32)
            for ref in ins[1:]:
                total += ref[...].astype(F32)
            flat[...] = total.astype(BF16)
            tall[...] = total.T.astype(BF16)

        flat, tall = kernel_call(
            sum_z_body, [((HD, piece), BF16), ((piece, HD), BF16)], head_at, own_head, flops=10**6
        )

        rows_here = [flat if (my, mx) == (0, 0) else send(flat, my=my, mx=mx) for my, mx in yx]
        rows_all = rows_here + [send(part, mc=1) for part in rows_here]
        tall_z = [tall] + [send(tall, mz=mz) for mz in range(1, n_z)]
        tall_zx = {(mz, mx): tall_z[mz] if mx == 0 else send(tall_z[mz], mx=mx) for mz in range(n_z) for mx in range(n_x)}

        def newton_schulz_body(at, *refs):
            ins, out = refs[:-1], refs[-1]
            raw = jnp.zeros((HD, HD), F32)
            for ref in ins:
                raw += lax.dot_general(ref[...], ref[...], NT, preferred_element_type=F32)
            down = lax.broadcasted_iota(jnp.int32, (HD, HD), 0)
            across = lax.broadcasted_iota(jnp.int32, (HD, HD), 1)
            identity = (down == across).astype(F32)
            divisor = jnp.sqrt(jnp.sum(raw * identity, keepdims=True)) + epsilon
            gram = raw / (divisor * divisor)
            total = None
            for step in range(NS_ITERS):
                factor = coef_a * identity + coef_b * gram + coef_c * exact_dot(gram, gram)
                total = factor if total is None else exact_dot(total, factor)
                if step + 1 < NS_ITERS:
                    gram = exact_dot(factor, exact_dot(gram, factor))
            out[...] = (0.2 * math.sqrt(din)) * (total / divisor)

        (total,) = kernel_call(
            newton_schulz_body,
            [((HD, HD), F32)],
            head_at,
            rows_all,
            flops=2 * HD * HD * HD * 6 * 20,
        )
        totals = [total] + [send(total, mz=mz) for mz in range(1, n_z)]

        weight_pieces, weight_at = [], []
        weight_near = {0: value_weight}
        weight_near[1] = send(value_weight, mc=1)
        for mc in range(CORES):
            weight_pieces.append(weight_near[mc])
            weight_at.append((y * CORES + source(core, mc, CORES)) * local_rows)
        for my in range(1, n_y):
            for mx in range(n_x):
                part = weight_far[my] if mx == 0 else send(weight_far[my], mx=mx)
                for mc in range(CORES):
                    weight_pieces.append(part if mc == 0 else send(part, mc=mc))
                    weight_at.append(
                        (source(y, my, n_y) * CORES + source(core, mc, CORES)) * local_rows
                        + source(x, mx, n_x) * piece
                    )

        def input_grad_body(at, cot, *refs):
            ins, out = refs[:-1], refs[-1]
            for k, ref in enumerate(ins):
                start = pl.multiple_of(at[k], LANES)
                out[:, pl.ds(start, ref.shape[0])] = lax.dot_general(
                    cot[...], ref[...], NT, preferred_element_type=F32
                ).astype(BF16)

        (input_grad,) = kernel_call(
            input_grad_body,
            [((tokens.shape[0], din), BF16)],
            jnp.stack(weight_at).astype(jnp.int32),
            [cotangent] + weight_pieces,
            flops=2 * tokens.shape[0] * din * width,
        )

        cols = [source(z, mz, n_z) * HD for mz in range(n_z)]
        rows_at = [source(x, mx, n_x) * piece for mx in range(n_x)]

        def update_body(at, *refs):
            mats, parts, out = refs[:n_z], refs[n_z:-1], refs[-1]
            for mz in range(n_z):
                high = mats[mz][...].astype(BF16)
                rest = mats[mz][...] - high.astype(F32)
                mid = rest.astype(BF16)
                low = (rest - mid.astype(F32)).astype(BF16)
                lanes = pl.ds(pl.multiple_of(at[mz], HD), HD)
                for mx in range(n_x):
                    part = parts[mz * n_x + mx][...]
                    value = lax.dot_general(part, high, NN, preferred_element_type=F32)
                    value += lax.dot_general(part, mid, NN, preferred_element_type=F32)
                    value += lax.dot_general(part, low, NN, preferred_element_type=F32)
                    out[pl.ds(pl.multiple_of(at[n_z + mx], 8), piece), lanes] = value

        (update,) = kernel_call(
            update_body,
            [((local_rows, width), F32)],
            jnp.stack(cols + rows_at).astype(jnp.int32),
            totals + [tall_zx[(mz, mx)] for mz in range(n_z) for mx in range(n_x)],
            flops=2 * local_rows * width * HD * 3,
        )
        return (input_grad, update)

    return per_device


def solution(mesh):
    in_specs = (P(("node", "rep"), None), P(("node", "rep"), None), P("node", None))
    out_specs = (P(("node", "rep"), None), P("node", None))

    def run(tokens, cotangent, value_weight):
        nodes, reps = mesh.shape["node"], mesh.shape["rep"]
        heads = value_weight.shape[1] // HD
        local_rows = value_weight.shape[0] // nodes
        fits = nodes % CORES == 0 and reps % heads == 0 and local_rows % (LANES * (reps // heads)) == 0
        body = exchanged(mesh) if fits else plain
        return jax.shard_map(
            body, mesh=mesh, in_specs=in_specs, out_specs=out_specs, check_vma=False
        )(tokens, cotangent, value_weight)

    return run
```
